32 devices in a mesh: wide: 8 (over z, x), narrow: 4 (over y, core).
Axes of the slice: x: 2, y: 2, z: 4, core: 2. Of those that a mesh axis runs over, the one named last changes fastest.
Arguments:
- hidden: bfloat16 [512, 4, 8192], P('narrow', None, 'wide'), may hold values from -0.1796875 to 0.1796875
- grad_out: bfloat16 [512, 8192], P('narrow', 'wide'), may hold values from -6 to 6
- weight_base: bfloat16 [32768, 8192], P('narrow', 'wide'), may hold values from -0.0625 to 0.0625
- block_scale: bfloat16 [2048, 512], P('narrow', 'wide'), may hold values from 0.25 to 4
Outputs:
- grad_hidden: bfloat16 [512, 4, 8192], P('narrow', None, 'wide')
- grad_weight: bfloat16 [8192, 4, 8192], P('narrow', None, 'wide')
The draws below stay inside these ranges and needn't reach their ends.
All inputs are finite; a program needn't handle non-finite values.
Results may differ from the reference program's by a relative error of at most 0.0049.
Values may be sent and summed in bfloat16 or wider, within the bound.
A program may use at most 512 MiB of HBM per device.

```python
import math
import jax
import jax.numpy as jnp

D = 8192
FF = 32768
BLOCK = 16
TOKENS = 512
GROUPS = 4
FGROUP = 8192


def shard_levels(rng, extent, pieces, least, largest):
    def one(dim, shards_of):
        heights = jax.random.uniform(jax.random.fold_in(jax.random.fold_in(rng, 6), dim), (shards_of,), jnp.float32, least / len(pieces), largest / len(pieces))
        return jnp.repeat(jnp.exp(heights), extent[dim] // shards_of).reshape((-1,) + (1,) * (len(extent) - dim - 1))

    loudness = one(*pieces[0])
    for cut in pieces[1:]:
        loudness = loudness * one(*cut)
    return loudness


def noise(own_key, extent, deviation, reach, cuts=(), dtype=jnp.bfloat16):
    loudness = shard_levels(own_key, extent, cuts, -0.22, 0.18) if cuts else 1.0
    entries = jax.random.normal(own_key, extent, jnp.float32) * deviation * loudness
    return jnp.minimum(jnp.maximum(entries, -reach), reach).astype(dtype)


def setup_inputs(seed: int = 0) -> dict:
    streams_of = jax.random.split(jax.random.key(seed), 5)
    return {
        "hidden": noise(streams_of[0], (TOKENS, GROUPS, FGROUP), 0.03, 0.1796875, ((0, 4), (2, 8))),
        "grad_out": noise(streams_of[1], (TOKENS, D), 1.0, 6.0, ((0, 4), (1, 8))),
        "weight_base": noise(streams_of[2], (FF, D), D ** -0.5, 0.0625, ((0, 4), (1, 8))),
        "block_scale": jnp.clip(jnp.exp(math.log(4.0) - 2.7725887 * jax.random.uniform(streams_of[3], (FF // BLOCK, D // BLOCK), jnp.float32) ** shard_levels(streams_of[3], (FF // BLOCK, D // BLOCK), ((0, 4), (1, 8)), -0.2, 0.2)), 0.25, 4.0).astype(jnp.bfloat16),
    }


def apply_scales(values, scales):
    height, breadth = values.shape
    widened = jnp.repeat(scales, 16, axis=1).astype(jnp.float32)
    blocked = values.reshape(height // 16, 16, breadth).astype(jnp.float32)
    blocked = blocked * widened[:, None, :]
    return blocked.reshape(height, breadth).astype(jnp.bfloat16)


def reference(hidden, grad_out, weight_base, block_scale):
    effective = apply_scales(weight_base, block_scale)
    flat_hidden = hidden.reshape(hidden.shape[0], hidden.shape[1] * hidden.shape[2])
    grad_flat = jnp.dot(grad_out, effective.T, preferred_element_type=jnp.float32)
    grad_hidden = grad_flat.astype(jnp.bfloat16).reshape(hidden.shape)
    grad_weight = jnp.dot(grad_out.T, flat_hidden, preferred_element_type=jnp.float32)
    grad_weight = grad_weight.astype(jnp.bfloat16).reshape(grad_out.shape[1], hidden.shape[1], hidden.shape[2])
    return grad_hidden, grad_weight
```

```python
import functools

import jax
import jax.numpy as jnp
from jax import lax
from jax.experimental import pallas as pl
from jax.experimental.pallas import tpu as pltpu
from jax.sharding import PartitionSpec as P

MESH = pl.DeviceIdType.MESH
BLOCK = 16
F32 = jnp.float32
BF16 = jnp.bfloat16


def loop(count, body):
    def step(i, carry):
        body(i)
        return carry

    lax.fori_loop(0, count, step, 0)


def add_into(dst, sources, rows):
    def step(i):
        at = pl.ds(pl.multiple_of(i * 16, 16), 16)
        total = sources[0][at, :].astype(F32)
        for source in sources[1:]:
            total = total + source[at, :].astype(F32)
        dst[at, :] = total.astype(BF16)

    loop(rows // 16, step)


def exchange_kernel(
    q, p, ra, scale_ref, weight_ref, grad_ref, hidden_ref,
    gh_ref, cols_ref, hall_ref,
    weff, s32, grads, hid, pa, pb, xr, ud, udb, xrb, fin,
    w_sem, l_sem, ag_s, ag_r, hd_s, hd_r, xa_s, xa_r, ud_s, ud_r, ub_s, ub_r,
    xb_s, xb_r, gh_s, gh_r, mz_s, mz_r, mx_s, mx_r,
):
    wide = q * p
    wi = lax.axis_index("wide")
    n = lax.axis_index("narrow")
    z = wi // p
    x = wi % p
    tokens = grads.shape[1]
    rb = tokens - ra
    high = (2 * z) // q

    def twin(k):
        a, b = n % 2, n // 2
        ka, kb = k % 2, k // 2
        return ((a + ka) % 2) + 2 * ((b + kb) % 2)

    def remote(src, dst, send, recv, to):
        return pltpu.make_async_remote_copy(
            src_ref=src, dst_ref=dst, send_sem=send, recv_sem=recv,
            device_id=to, device_id_type=MESH)

    def at_zx(zz, xx):
        return (zz * p + xx, n)

    def order(i, d):
        return i + (1 - d) * (q - 1 - 2 * i)

    own_grad = pltpu.make_async_copy(grad_ref, grads.at[0], l_sem.at[0])
    own_grad.start()
    own_hid = pltpu.make_async_copy(hidden_ref, hid, l_sem.at[1])
    own_hid.start()

    def weight_copy(c):
        return pltpu.make_async_copy(weight_ref.at[c], weff.at[c], w_sem.at[c])

    def start_weights(i):
        loop(p, lambda xx: weight_copy(order(i, high) * p + xx).start())

    loop(q, start_weights)

    barrier = pltpu.get_barrier_semaphore()

    def greet(device):
        pl.semaphore_signal(barrier, inc=1, device_id=device, device_id_type=MESH)

    for k in range(1, q):
        greet((wi, twin(k)))
    loop(p - 1, lambda r: greet(at_zx(z, (x + 1 + r) % p)))

    @pl.when(z > 0)
    def _():
        greet(at_zx(z - 1, x))

    @pl.when(z < q - 1)
    def _():
        greet(at_zx(z + 1, x))

    ends = (z == 0) | (z == q - 1)

    @pl.when(ends)
    def _():
        pl.semaphore_wait(barrier, q + p - 1)

    @pl.when(jnp.logical_not(ends))
    def _():
        pl.semaphore_wait(barrier, q + p)

    def ag_copy(k):
        return remote(grads.at[0], grads.at[k], ag_s.at[k], ag_r.at[k], (wi, twin(k)))

    def hid_copy(k):
        return remote(hid, hall_ref.at[k], hd_s.at[k], hd_r.at[k], (wi, twin(k)))

    own_grad.wait()
    for k in (2, 3, 1):
        ag_copy(k).start()

    features = weff.shape[2]
    blocks = features // BLOCK
    row = lax.broadcasted_iota(jnp.int32, (blocks, features), 0)
    col = lax.broadcasted_iota(jnp.int32, (blocks, features), 1)
    low = row * BLOCK
    spread = jnp.where((col >= low) & (col < low + BLOCK), 1.0, 0.0).astype(BF16)
    s32[...] = lax.dot_general(
        scale_ref[...], spread, (((0,), (0,)), ((), ())), preferred_element_type=F32)

    own_hid.wait()
    for k in (2, 3, 1):
        hid_copy(k).start()
    hid_here = pltpu.make_async_copy(hid, hall_ref.at[0], l_sem.at[1])
    hid_here.start()

    units = weff.shape[1]
    per_chunk = units // BLOCK

    def scale_chunk(c):
        weight_copy(c).wait()

        def step(i):
            at = pl.ds(pl.multiple_of(i * BLOCK, BLOCK), BLOCK)
            factor = s32[pl.ds(c * per_chunk + i, 1), :]
            weff[c, at, :] = (weff[c, at, :].astype(F32) * factor).astype(BF16)

        loop(per_chunk, step)

    def xa_copy(b, zt, r):
        xx = (x + 1 + r) % p
        return remote(pa.at[b, zt, xx], xr.at[b, zt, r], xa_s.at[b, zt, r], xa_r.at[b, zt, r], at_zx(z, xx))

    def ud_copy(d, b, zt):
        return remote(ud.at[d, b, zt], ud.at[d, b, zt], ud_s.at[d, b, zt], ud_r.at[d, b, zt],
                      at_zx(z + 1 - 2 * d, x))

    def ub_copy(d, b, zt, src):
        return remote(src, udb.at[d, b, zt], ub_s.at[d, b, zt], ub_r.at[d, b, zt],
                      at_zx(z + 1 - 2 * d, x))

    def stage_x(b):
        def per_row(i):
            zt = order(i, high)

            def per_col(xx):
                c = zt * p + xx

                @pl.when(b == 0)
                def _():
                    scale_chunk(c)

                part = lax.dot_general(
                    grads[b], weff[c], (((1,), (1,)), ((), ())), preferred_element_type=F32
                ).astype(BF16)
                pa[b, zt, xx] = part[:ra]
                pb[b, zt, xx] = part[ra:]

            loop(p, per_col)
            loop(p - 1, lambda r: xa_copy(b, zt, r).start())
            for d in range(2):
                @pl.when((z == d * (q - 1)) & (zt != z))
                def _():
                    ub_copy(d, b, zt, pb.at[b, zt]).start()

        loop(q, per_row)

    def wait_x(b, zt):
        loop(p - 1, lambda r: xa_copy(b, zt, r).wait_recv())

    def x_sources(b, zt):
        return [pa.at[b, zt, x]] + [xr.at[b, zt, r] for r in range(p - 1)]

    def stage_z(b):
        for ph in range(2):
            d = (ph + high) % 2
            sign = 1 - 2 * d
            edge = d * (q - 1)

            def step_b(i):
                zt = order(i, d)

                @pl.when(((zt - z) * sign > 0) & (z != edge))
                def _():
                    copy = ub_copy(d, b, zt, udb.at[d, b, zt])
                    copy.wait_recv()
                    loop(p, lambda xx: add_into(
                        udb.at[d, b, zt, xx], [udb.at[d, b, zt, xx], pb.at[b, zt, xx]], rb))
                    copy.start()

            def step_a(i):
                zt = order(i, d)

                @pl.when((zt - z) * sign > 0)
                def _():
                    wait_x(b, zt)
                    copy = ud_copy(d, b, zt)

                    @pl.when(z != edge)
                    def _():
                        copy.wait_recv()
                        add_into(ud.at[d, b, zt], [ud.at[d, b, zt]] + x_sources(b, zt), ra)

                    @pl.when(z == edge)
                    def _():
                        add_into(ud.at[d, b, zt], x_sources(b, zt), ra)

                    copy.start()

            loop(q, step_b)
            loop(q, step_a)

    def xb_copy(b, r):
        xx = (x + 1 + r) % p
        return remote(pb.at[b, z, xx], xrb.at[b, r], xb_s.at[b, r], xb_r.at[b, r], at_zx(z, xx))

    def stage_f1(b):
        for d in range(2):
            @pl.when(z != d * (q - 1))
            def _():
                ub_copy(d, b, z, udb.at[d, b, z]).wait_recv()
                loop(p, lambda xx: add_into(
                    pb.at[b, z, xx], [pb.at[b, z, xx], udb.at[d, b, z, xx]], rb))
        loop(p - 1, lambda r: xb_copy(b, r).start())

        wait_x(b, z)
        for d in range(2):
            @pl.when(z != d * (q - 1))
            def _():
                ud_copy(d, b, z).wait_recv()
        out = fin.at[b, pl.ds(0, ra)]

        @pl.when(z == 0)
        def _():
            add_into(out, x_sources(b, z) + [ud.at[1, b, z]], ra)

        @pl.when(z == q - 1)
        def _():
            add_into(out, x_sources(b, z) + [ud.at[0, b, z]], ra)

        @pl.when((z > 0) & (z < q - 1))
        def _():
            add_into(out, x_sources(b, z) + [ud.at[0, b, z], ud.at[1, b, z]], ra)

    def gh_copy(b):
        return remote(fin.at[b], gh_ref.at[n], gh_s.at[b], gh_r.at[b], (wi, twin(b)))

    def gh_here():
        return pltpu.make_async_copy(fin.at[0], gh_ref.at[n], l_sem.at[0])

    def stage_f2(b):
        loop(p - 1, lambda r: xb_copy(b, r).wait_recv())
        add_into(fin.at[b, pl.ds(ra, rb)],
                 [pb.at[b, z, x]] + [xrb.at[b, r] for r in range(p - 1)], rb)

        @pl.when(b == 0)
        def _():
            gh_here().start()

        @pl.when(b != 0)
        def _():
            gh_copy(b).start()

    def mz_copy(k, d, src):
        return remote(src, cols_ref.at[x, k], mz_s.at[d, k], mz_r.at[k], at_zx(z + 1 - 2 * d, x))

    def mx_copy(k, r, src):
        return remote(src, cols_ref.at[x, k], mx_s.at[k, r], mx_r.at[k, r], at_zx(z, (x + 1 + r) % p))

    def cols_here(k):
        return pltpu.make_async_copy(grads.at[k], cols_ref.at[x, k], w_sem.at[k])

    def multicast_source(k):
        @pl.when(z == n)
        def _():
            cols_here(k).start()
            for d in range(2):
                @pl.when(z != (1 - d) * (q - 1))
                def _():
                    mz_copy(k, d, grads.at[k]).start()

    def multicast_relay(k):
        @pl.when(z == n)
        def _():
            loop(p - 1, lambda r: mx_copy(k, r, grads.at[k]).start())

        for d in range(2):
            @pl.when((z - n) * (1 - 2 * d) > 0)
            def _():
                mz_copy(k, d, cols_ref.at[x, k]).wait_recv()

                @pl.when(z != (1 - d) * (q - 1))
                def _():
                    mz_copy(k, d, cols_ref.at[x, k]).start()

                loop(p - 1, lambda r: mx_copy(k, r, cols_ref.at[x, k]).start())

    def stage(s):
        @pl.when(s < q)
        def _():
            @pl.when(s == 1)
            def _():
                for k in range(1, q):
                    ag_copy(k).wait_recv()
                for k in range(q):
                    multicast_source(k)

            stage_x(s)

        @pl.when((s >= 1) & (s <= q))
        def _():
            stage_z(s - 1)
            @pl.when(s == 1)
            def _():
                for k in range(q // 2):
                    multicast_relay(k)

            @pl.when(s == 2)
            def _():
                for k in range(q // 2, q):
                    multicast_relay(k)

        @pl.when((s >= 2) & (s <= q + 1))
        def _():
            stage_f1(s - 2)

        @pl.when((s >= 3) & (s <= q + 2))
        def _():
            stage_f2(s - 3)

    loop(q + 3, stage)

    for k in range(1, q):
        ag_copy(k).wait_send()
        hid_copy(k).wait()
        gh_copy(k).wait()
    hid_here.wait()
    gh_here().wait()

    def drain_b(b):
        loop(p - 1, lambda r: xb_copy(b, r).wait_send())

        def per_row(zt):
            loop(p - 1, lambda r: xa_copy(b, zt, r).wait_send())
            for d in range(2):
                @pl.when((zt - z) * (1 - 2 * d) > 0)
                def _():
                    ud_copy(d, b, zt).wait_send()
                    ub_copy(d, b, zt, udb.at[d, b, zt]).wait_send()

        loop(q, per_row)

        @pl.when(z == n)
        def _():
            cols_here(b).wait()

        for d in range(2):
            @pl.when(((z - n) * (1 - 2 * d) >= 0) & (z != (1 - d) * (q - 1)))
            def _():
                mz_copy(b, d, cols_ref.at[x, b]).wait_send()
        loop(p - 1, lambda r: mx_copy(b, r, cols_ref.at[x, b]).wait())

    loop(q, drain_b)


def exchange(wide, narrow, hidden, grad_out, weight, scale_t):
    q = narrow
    p = wide // narrow
    tokens, features = grad_out.shape
    units = weight.shape[1]
    ra = tokens * 3 // 4 // 16 * 16
    rb = tokens - ra
    dma = pltpu.SemaphoreType.DMA
    any_space = pl.BlockSpec(memory_space=pl.ANY)
    vm = pl.BlockSpec(memory_space=pltpu.VMEM)
    return pl.pallas_call(
        functools.partial(exchange_kernel, q, p, ra),
        out_shape=(
            jax.ShapeDtypeStruct((narrow, tokens, units), BF16),
            jax.ShapeDtypeStruct((p, q, tokens, features), BF16),
            jax.ShapeDtypeStruct((q,) + hidden.shape, BF16),
        ),
        in_specs=[vm, any_space, any_space, any_space],
        out_specs=(any_space, any_space, any_space),
        scratch_shapes=[
            pltpu.VMEM((wide, units, features), BF16),
            pltpu.VMEM((scale_t.shape[1], features), F32),
            pltpu.VMEM((q, tokens, features), BF16),
            pltpu.VMEM(hidden.shape, BF16),
            pltpu.VMEM((q, q, p, ra, units), BF16),
            pltpu.VMEM((q, q, p, rb, units), BF16),
            pltpu.VMEM((q, q, p - 1, ra, units), BF16),
            pltpu.VMEM((2, q, q, ra, units), BF16),
            pltpu.VMEM((2, q, q, p, rb, units), BF16),
            pltpu.VMEM((q, p - 1, rb, units), BF16),
            pltpu.VMEM((q, tokens, units), BF16),
            dma((wide,)), dma((2,)), dma((q,)), dma((q,)), dma((q,)), dma((q,)),
            dma((q, q, p - 1)), dma((q, q, p - 1)),
            dma((2, q, q)), dma((2, q, q)), dma((2, q, q)), dma((2, q, q)),
            dma((q, p - 1)), dma((q, p - 1)), dma((q,)), dma((q,)),
            dma((2, q)), dma((q,)), dma((q, p - 1)), dma((q, p - 1)),
        ],
        compiler_params=pltpu.CompilerParams(
            collective_id=0, has_side_effects=True, vmem_limit_bytes=62 * 1024 * 1024),
        name="exchange",
    )(scale_t, weight, grad_out, hidden)


def outer_kernel(groups, units, cols_ref, hidden_ref, out_ref):
    for g in range(groups):
        part = lax.dot_general(
            cols_ref[0], hidden_ref[:, g * units:(g + 1) * units],
            (((0,), (0,)), ((), ())), preferred_element_type=F32)
        out_ref[:, g, :] = part.astype(BF16)


def outer_product(cols, hidden, groups):
    p, tokens, features = cols.shape
    units = hidden.shape[1] // groups
    rows = min(256, features)
    steps = features // rows
    return pl.pallas_call(
        functools.partial(outer_kernel, groups, units),
        grid=(p, steps),
        out_shape=jax.ShapeDtypeStruct((p * features, groups, units), BF16),
        in_specs=[
            pl.BlockSpec((1, tokens, rows), lambda i, j: (i, 0, j)),
            pl.BlockSpec(hidden.shape, lambda i, j: (0, 0), pipeline_mode=pl.Buffered(1)),
        ],
        out_specs=pl.BlockSpec((rows, groups, units), lambda i, j: (i * steps + j, 0, 0)),
        compiler_params=pltpu.CompilerParams(vmem_limit_bytes=60 * 1024 * 1024),
        name="outer_product",
    )(cols, hidden)


def per_device(wide, narrow, hidden, grad_out, weight_base, block_scale):
    tokens, groups, units = hidden.shape
    features = grad_out.shape[1]
    flat = hidden.reshape(tokens, groups * units)
    weight = weight_base.reshape(wide, weight_base.shape[0] // wide, features)
    gh, cols, hall = exchange(wide, narrow, flat, grad_out, weight, block_scale.T)
    grad_hidden = gh.transpose(1, 0, 2)
    p = cols.shape[0]
    every = narrow * tokens
    grad_weight = outer_product(
        cols.reshape(p, every, features), hall.reshape(every, groups * units), groups)
    return grad_hidden, grad_weight


def solution(mesh):
    wide, narrow = mesh.shape["wide"], mesh.shape["narrow"]
    return jax.shard_map(
        functools.partial(per_device, wide, narrow),
        mesh=mesh,
        in_specs=(P("narrow", None, "wide"), P("narrow", "wide"), P("narrow", "wide"), P("narrow", "wide")),
        out_specs=(P("narrow", None, "wide"), P("narrow", None, "wide")),
        check_vma=False,
    )
```

```python
import functools

import jax
import jax.numpy as jnp
from jax import lax
from jax.experimental import pallas as pl
from jax.experimental.pallas import tpu as pltpu
from jax.sharding import PartitionSpec as P

MESH = pl.DeviceIdType.MESH
BLOCK = 16
F32 = jnp.float32
BF16 = jnp.bfloat16


def loop(count, body, unroll=1):
    def step(i, carry):
        body(i)
        return carry

    lax.fori_loop(0, count, step, 0, unroll=unroll)


def add_into(dst, sources, rows):
    def step(i):
        at = pl.ds(pl.multiple_of(i * 16, 16), 16)
        total = sources[0][at, :].astype(F32)
        for source in sources[1:]:
            total = total + source[at, :].astype(F32)
        dst[at, :] = total.astype(BF16)

    loop(rows // 16, step)


def exchange_kernel(
    q, p, ra, scale_ref, weight_ref, grad_ref, hidden_ref,
    gh_ref, cols_ref, hall_ref,
    weff, s32, grads, raw, hid, pa, pb, xr, ud, udb, xrb, fin,
    w_sem, l_sem, ag_s, ag_r, hd_s, hd_r, xa_s, xa_r, ud_s, ud_r, ub_s, ub_r,
    xb_s, xb_r, gh_s, gh_r, mz_s, mz_r, mx_s, mx_r, own_sem,
):
    wide = q * p
    wi = lax.axis_index("wide")
    n = lax.axis_index("narrow")
    z = wi // p
    x = wi % p
    tokens = grads.shape[1]
    rb = tokens - ra
    high = (2 * z) // q

    def twin(k):
        a, b = k // 2, (k % 2 + k // 2) % 2
        return ((n % 2 + a) % 2) + 2 * ((n // 2 + b) % 2)

    def remote(src, dst, send, recv, to):
        return pltpu.make_async_remote_copy(
            src_ref=src, dst_ref=dst, send_sem=send, recv_sem=recv,
            device_id=to, device_id_type=MESH)

    def at_zx(zz, xx):
        return (zz * p + xx, n)

    def order(i, d):
        return i + (1 - d) * (q - 1 - 2 * i)

    own_grad = pltpu.make_async_copy(grad_ref, grads.at[0], l_sem.at[0])
    own_grad.start()
    own_hid = pltpu.make_async_copy(hidden_ref, raw, l_sem.at[1])
    own_hid.start()

    def weight_copy(c):
        return pltpu.make_async_copy(weight_ref.at[c], weff.at[c], w_sem.at[c])

    def start_weights(i):
        loop(p, lambda xx: weight_copy(order(i, high) * p + xx).start())

    loop(q, start_weights)

    barrier = pltpu.get_barrier_semaphore()

    def greet(device):
        pl.semaphore_signal(barrier, inc=1, device_id=device, device_id_type=MESH)

    for k in range(1, q):
        greet((wi, twin(k)))
    loop(p - 1, lambda r: greet(at_zx(z, (x + 1 + r) % p)))

    @pl.when(z > 0)
    def _():
        greet(at_zx(z - 1, x))

    @pl.when(z < q - 1)
    def _():
        greet(at_zx(z + 1, x))

    ends = (z == 0) | (z == q - 1)

    @pl.when(ends)
    def _():
        pl.semaphore_wait(barrier, q + p - 1)

    @pl.when(jnp.logical_not(ends))
    def _():
        pl.semaphore_wait(barrier, q + p)

    def ag_copy(k):
        return remote(grads.at[0], grads.at[k], ag_s.at[k], ag_r.at[k], (wi, twin(k)))

    def hid_copy(k):
        return remote(hid, hall_ref.at[k], hd_s.at[k], hd_r.at[k], (wi, twin(k)))

    def hid_here():
        return pltpu.make_async_copy(hid, hall_ref.at[0], l_sem.at[1])

    def share_hidden():
        own_hid.wait()
        groups, width = raw.shape[1:]

        def step(i):
            at = pl.ds(pl.multiple_of(i * 16, 16), 16)
            for g in range(groups):
                hid[at, g * width:(g + 1) * width] = raw[at, g, :]

        loop(raw.shape[0] // 16, step)
        for k in range(1, q):
            hid_copy(k).start()
        hid_here().start()

    own_grad.wait()
    for k in range(1, q):
        ag_copy(k).start()

    features = weff.shape[2]
    blocks = features // BLOCK
    row = lax.broadcasted_iota(jnp.int32, (blocks, features), 0)
    col = lax.broadcasted_iota(jnp.int32, (blocks, features), 1)
    low = row * BLOCK
    spread = jnp.where((col >= low) & (col < low + BLOCK), 1.0, 0.0).astype(BF16)
    s32[...] = lax.dot_general(
        scale_ref[...], spread, (((0,), (0,)), ((), ())), preferred_element_type=F32)

    units = weff.shape[1]
    per_chunk = units // BLOCK

    def scale_chunk(c):
        weight_copy(c).wait()

        def step(i):
            at = pl.ds(pl.multiple_of(i * BLOCK, BLOCK), BLOCK)
            factor = s32[pl.ds(c * per_chunk + i, 1), :]
            weff[c, at, :] = (weff[c, at, :].astype(F32) * factor).astype(BF16)

        loop(per_chunk, step, 4)

    def xa_copy(b, zt, r):
        xx = (x + 1 + r) % p
        return remote(pa.at[b, zt, xx], xr.at[b, zt, r], xa_s.at[b, zt, r], xa_r.at[b, zt, r], at_zx(z, xx))

    def ud_copy(d, b, zt):
        return remote(ud.at[d, b, zt], ud.at[d, b, zt], ud_s.at[d, b, zt], ud_r.at[d, b, zt],
                      at_zx(z + 1 - 2 * d, x))

    def ub_copy(d, b, zt, src):
        return remote(src, udb.at[d, b, zt], ub_s.at[d, b, zt], ub_r.at[d, b, zt],
                      at_zx(z + 1 - 2 * d, x))

    def send_row(b, zt):
        loop(p - 1, lambda r: xa_copy(b, zt, r).start())
        for d in range(2):
            @pl.when((z == d * (q - 1)) & (zt != z))
            def _():
                ub_copy(d, b, zt, pb.at[b, zt]).start()

    def keep(b, zt, xx, part):
        pa[b, zt, xx] = part[:ra]
        pb[b, zt, xx] = part[ra:]

    def first_rows(i):
        zt = order(i, high)

        def per_col(xx):
            c = zt * p + xx
            scale_chunk(c)
            keep(0, zt, xx, lax.dot_general(
                grads[0], weff[c], (((1,), (1,)), ((), ())), preferred_element_type=F32
            ).astype(BF16))

        loop(p, per_col)
        send_row(0, zt)

    def other_rows(i):
        zt = order(i, high)

        def per_col(xx):
            part = lax.dot_general(
                grads[1:].reshape((q - 1) * tokens, features), weff[zt * p + xx],
                (((1,), (1,)), ((), ())), preferred_element_type=F32).astype(BF16)
            for b in range(1, q):
                keep(b, zt, xx, part[(b - 1) * tokens:b * tokens])

        loop(p, per_col)
        send_row(1, zt)

    def wait_x(b, zt):
        loop(p - 1, lambda r: xa_copy(b, zt, r).wait_recv())

    def x_sources(b, zt):
        return [pa.at[b, zt, x]] + [xr.at[b, zt, r] for r in range(p - 1)]

    def stage_zb(b):
        for ph in range(2):
            d = (ph + high) % 2

            def step_b(i):
                zt = order(i, d)

                @pl.when(((zt - z) * (1 - 2 * d) > 0) & (z != d * (q - 1)))
                def _():
                    copy = ub_copy(d, b, zt, udb.at[d, b, zt])
                    copy.wait_recv()
                    loop(p, lambda xx: add_into(
                        udb.at[d, b, zt, xx], [udb.at[d, b, zt, xx], pb.at[b, zt, xx]], rb))
                    copy.start()

            loop(q, step_b)

    def stage_za(b):
        for ph in range(2):
            d = (ph + high) % 2
            edge = d * (q - 1)

            def step_a(i):
                zt = order(i, d)

                @pl.when((zt - z) * (1 - 2 * d) > 0)
                def _():
                    wait_x(b, zt)
                    copy = ud_copy(d, b, zt)

                    @pl.when(z != edge)
                    def _():
                        copy.wait_recv()
                        add_into(ud.at[d, b, zt], [ud.at[d, b, zt]] + x_sources(b, zt), ra)

                    @pl.when(z == edge)
                    def _():
                        add_into(ud.at[d, b, zt], x_sources(b, zt), ra)

                    copy.start()

            loop(q, step_a)

    def xb_copy(b, r):
        xx = (x + 1 + r) % p
        return remote(pb.at[b, z, xx], xrb.at[b, r], xb_s.at[b, r], xb_r.at[b, r], at_zx(z, xx))

    def stage_f1(b):
        for d in range(2):
            @pl.when(z != d * (q - 1))
            def _():
                ub_copy(d, b, z, udb.at[d, b, z]).wait_recv()
                loop(p, lambda xx: add_into(
                    pb.at[b, z, xx], [pb.at[b, z, xx], udb.at[d, b, z, xx]], rb))
        loop(p - 1, lambda r: xb_copy(b, r).start())

        wait_x(b, z)
        for d in range(2):
            @pl.when(z != d * (q - 1))
            def _():
                ud_copy(d, b, z).wait_recv()
        out = fin.at[b, pl.ds(0, ra)]

        @pl.when(z == 0)
        def _():
            add_into(out, x_sources(b, z) + [ud.at[1, b, z]], ra)

        @pl.when(z == q - 1)
        def _():
            add_into(out, x_sources(b, z) + [ud.at[0, b, z]], ra)

        @pl.when((z > 0) & (z < q - 1))
        def _():
            add_into(out, x_sources(b, z) + [ud.at[0, b, z], ud.at[1, b, z]], ra)

    def gh_copy(b):
        return remote(fin.at[b], gh_ref.at[n], gh_s.at[b], gh_r.at[b], (wi, twin(b)))

    def gh_here():
        return pltpu.make_async_copy(fin.at[0], gh_ref.at[n], l_sem.at[0])

    def stage_f2(b):
        loop(p - 1, lambda r: xb_copy(b, r).wait_recv())
        add_into(fin.at[b, pl.ds(ra, rb)],
                 [pb.at[b, z, x]] + [xrb.at[b, r] for r in range(p - 1)], rb)

        @pl.when(b == 0)
        def _():
            gh_here().start()

        @pl.when(b != 0)
        def _():
            gh_copy(b).start()

    def mz_copy(k, d, src):
        return remote(src, cols_ref.at[x, k], mz_s.at[d, k], mz_r.at[k], at_zx(z + 1 - 2 * d, x))

    def mx_copy(k, r, src):
        return remote(src, cols_ref.at[x, k], mx_s.at[k, r], mx_r.at[k, r], at_zx(z, (x + 1 + r) % p))

    def cols_here(k):
        return pltpu.make_async_copy(grads.at[k], cols_ref.at[x, k], own_sem.at[k])

    def multicast_source(k):
        @pl.when(z == n)
        def _():
            cols_here(k).start()
            for d in range(2):
                @pl.when(z != (1 - d) * (q - 1))
                def _():
                    mz_copy(k, d, grads.at[k]).start()

    def multicast_relay(k):
        @pl.when(z == n)
        def _():
            loop(p - 1, lambda r: mx_copy(k, r, grads.at[k]).start())

        for d in range(2):
            @pl.when((z - n) * (1 - 2 * d) > 0)
            def _():
                mz_copy(k, d, cols_ref.at[x, k]).wait_recv()

                @pl.when(z != (1 - d) * (q - 1))
                def _():
                    mz_copy(k, d, cols_ref.at[x, k]).start()

                loop(p - 1, lambda r: mx_copy(k, r, cols_ref.at[x, k]).start())

    multicast_source(0)
    ag_copy(q - 1).wait_recv()
    multicast_source(q - 1)
    loop(q, first_rows)
    for k in range(1, q - 1):
        ag_copy(k).wait_recv()
        multicast_source(k)
    loop(q, other_rows)
    loop(q - 2, lambda b: loop(q, lambda i: send_row(b + 2, order(i, high))))
    share_hidden()
    loop(q, stage_zb)

    away = (z - n) * (z - n)
    inner = jnp.logical_not(ends)

    def relay_when(condition):
        @pl.when(condition)
        def _():
            loop(q, multicast_relay)

    relay_when((away == 0) | (inner & (away == 1)))
    loop(2, stage_za)
    relay_when(inner & (away > 1))
    loop(q - 2, lambda b: stage_za(b + 2))
    relay_when(ends & (away > 0))
    loop(q - 1, stage_f1)
    loop(q - 1, stage_f2)
    stage_f1(q - 1)
    stage_f2(q - 1)

    for k in range(1, q):
        ag_copy(k).wait_send()
        hid_copy(k).wait()
        gh_copy(k).wait()
    hid_here().wait()
    gh_here().wait()

    def drain_b(b):
        loop(p - 1, lambda r: xb_copy(b, r).wait_send())

        def per_row(zt):
            loop(p - 1, lambda r: xa_copy(b, zt, r).wait_send())
            for d in range(2):
                @pl.when((zt - z) * (1 - 2 * d) > 0)
                def _():
                    ud_copy(d, b, zt).wait_send()
                    ub_copy(d, b, zt, udb.at[d, b, zt]).wait_send()

        loop(q, per_row)

        @pl.when(z == n)
        def _():
            cols_here(b).wait()

        for d in range(2):
            @pl.when(((z - n) * (1 - 2 * d) >= 0) & (z != (1 - d) * (q - 1)))
            def _():
                mz_copy(b, d, cols_ref.at[x, b]).wait_send()
        loop(p - 1, lambda r: mx_copy(b, r, cols_ref.at[x, b]).wait())

    loop(q, drain_b)


def exchange(wide, narrow, hidden, grad_out, weight, scale_t):
    q = narrow
    p = wide // narrow
    tokens, features = grad_out.shape
    units = weight.shape[1]
    ra = tokens * 3 // 4 // 16 * 16
    rb = tokens - ra
    flat = (tokens, hidden.shape[1] * hidden.shape[2])
    dma = pltpu.SemaphoreType.DMA
    any_space = pl.BlockSpec(memory_space=pl.ANY)
    vm = pl.BlockSpec(memory_space=pltpu.VMEM)
    return pl.pallas_call(
        functools.partial(exchange_kernel, q, p, ra),
        out_shape=(
            jax.ShapeDtypeStruct((narrow, tokens, units), BF16),
            jax.ShapeDtypeStruct((p, q, tokens, features), BF16),
            jax.ShapeDtypeStruct((q,) + flat, BF16),
        ),
        in_specs=[vm, any_space, any_space, any_space],
        out_specs=(any_space, any_space, any_space),
        scratch_shapes=[
            pltpu.VMEM((wide, units, features), BF16),
            pltpu.VMEM((scale_t.shape[1], features), F32),
            pltpu.VMEM((q, tokens, features), BF16),
            pltpu.VMEM(hidden.shape, BF16),
            pltpu.VMEM(flat, BF16),
            pltpu.VMEM((q, q, p, ra, units), BF16),
            pltpu.VMEM((q, q, p, rb, units), BF16),
            pltpu.VMEM((q, q, p - 1, ra, units), BF16),
            pltpu.VMEM((2, q, q, ra, units), BF16),
            pltpu.VMEM((2, q, q, p, rb, units), BF16),
            pltpu.VMEM((q, p - 1, rb, units), BF16),
            pltpu.VMEM((q, tokens, units), BF16),
            dma((wide,)), dma((2,)), dma((q,)), dma((q,)), dma((q,)), dma((q,)),
            dma((q, q, p - 1)), dma((q, q, p - 1)),
            dma((2, q, q)), dma((2, q, q)), dma((2, q, q)), dma((2, q, q)),
            dma((q, p - 1)), dma((q, p - 1)), dma((q,)), dma((q,)),
            dma((2, q)), dma((q,)), dma((q, p - 1)), dma((q, p - 1)), dma((q,)),
        ],
        compiler_params=pltpu.CompilerParams(
            collective_id=0, has_side_effects=True, vmem_limit_bytes=62 * 1024 * 1024),
        name="exchange",
    )(scale_t, weight, grad_out, hidden)


def outer_kernel(groups, units, cols_ref, hidden_ref, gh_ref, out_ref, grad_hidden_ref, rows_ref):
    rows = cols_ref.shape[2]
    for g in range(groups):
        part = lax.dot_general(
            cols_ref[0], hidden_ref[:, g * units:(g + 1) * units],
            (((0,), (0,)), ((), ())), preferred_element_type=F32)
        for j in range(units // 128):
            rows_ref[j, pl.ds(g, rows, stride=groups), :] = part[:, j * 128:(j + 1) * 128]
    for j in range(units // 128):
        out_ref[:, :, j * 128:(j + 1) * 128] = rows_ref[j].astype(BF16).reshape(rows, groups, 128)
    for g in range(groups):
        grad_hidden_ref[:, g, :] = gh_ref[g]


def outer_product(cols, hidden, gh):
    p, tokens, features = cols.shape
    groups, own, units = gh.shape
    rows = min(256, features)
    steps = features // rows
    share = own // (p * steps)
    return pl.pallas_call(
        functools.partial(outer_kernel, groups, units),
        grid=(p, steps),
        out_shape=(
            jax.ShapeDtypeStruct((p * features, groups, units), BF16),
            jax.ShapeDtypeStruct((own, groups, units), BF16),
        ),
        in_specs=[
            pl.BlockSpec((1, tokens, rows), lambda i, j: (i, 0, j)),
            pl.BlockSpec(hidden.shape, lambda i, j: (0, 0), pipeline_mode=pl.Buffered(1)),
            pl.BlockSpec((groups, share, units), lambda i, j: (0, i * steps + j, 0)),
        ],
        out_specs=(
            pl.BlockSpec((rows, groups, units), lambda i, j: (i * steps + j, 0, 0)),
            pl.BlockSpec((share, groups, units), lambda i, j: (i * steps + j, 0, 0)),
        ),
        scratch_shapes=[pltpu.VMEM((units // 128, rows * groups, 128), F32)],
        compiler_params=pltpu.CompilerParams(vmem_limit_bytes=60 * 1024 * 1024),
        name="outer_product",
    )(cols, hidden, gh)


def per_device(wide, narrow, hidden, grad_out, weight_base, block_scale):
    tokens, groups, units = hidden.shape
    features = grad_out.shape[1]
    weight = weight_base.reshape(wide, weight_base.shape[0] // wide, features)
    gh, cols, hall = exchange(wide, narrow, hidden, grad_out, weight, block_scale.T)
    p = cols.shape[0]
    every = narrow * tokens
    grad_weight, grad_hidden = outer_product(
        cols.reshape(p, every, features), hall.reshape(every, groups * units), gh)
    return grad_hidden, grad_weight


def solution(mesh):
    wide, narrow = mesh.shape["wide"], mesh.shape["narrow"]
    return jax.shard_map(
        functools.partial(per_device, wide, narrow),
        mesh=mesh,
        in_specs=(P("narrow", None, "wide"), P("narrow", "wide"), P("narrow", "wide"), P("narrow", "wide")),
        out_specs=(P("narrow", None, "wide"), P("narrow", None, "wide")),
        check_vma=False,
    )
```

```python
import functools

import jax
import jax.numpy as jnp
from jax import lax
from jax.experimental import pallas as pl
from jax.experimental.pallas import tpu as pltpu
from jax.sharding import PartitionSpec as P

MESH = pl.DeviceIdType.MESH
BLOCK = 16
F32 = jnp.float32
BF16 = jnp.bfloat16


def loop(count, body, unroll=1):
    def step(i, carry):
        body(i)
        return carry

    lax.fori_loop(0, count, step, 0, unroll=unroll)


def add_into(dst, sources, rows):
    def step(i):
        at = pl.ds(pl.multiple_of(i * 16, 16), 16)
        total = sources[0][at, :].astype(F32)
        for source in sources[1:]:
            total = total + source[at, :].astype(F32)
        dst[at, :] = total.astype(BF16)

    loop(rows // 16, step)


def exchange_kernel(
    q, p, ra, scale_ref, weight_ref, grad_ref, hidden_ref,
    gh_ref, cols_ref, hall_ref,
    weff, s32, grads, raw, hid, pa, pb, xr, ud, udb, xrb, fin,
    w_sem, l_sem, ag_s, ag_r, hd_s, hd_r, xa_s, xa_r, ud_s, ud_r, ub_s, ub_r,
    xb_s, xb_r, gh_s, gh_r, mz_s, mz_r, mx_s, mx_r, own_sem,
):
    wide = q * p
    wi = lax.axis_index("wide")
    n = lax.axis_index("narrow")
    z = wi // p
    x = wi % p
    tokens = grads.shape[1]
    rb = tokens - ra
    high = (2 * z) // q

    def twin(k):
        a, b = k // 2, (k % 2 + k // 2) % 2
        return ((n % 2 + a) % 2) + 2 * ((n // 2 + b) % 2)

    def remote(src, dst, send, recv, to):
        return pltpu.make_async_remote_copy(
            src_ref=src, dst_ref=dst, send_sem=send, recv_sem=recv,
            device_id=to, device_id_type=MESH)

    def at_zx(zz, xx):
        return (zz * p + xx, n)

    def order(i, d):
        return i + (1 - d) * (q - 1 - 2 * i)

    own_grad = pltpu.make_async_copy(grad_ref, grads.at[0], l_sem.at[0])
    own_grad.start()
    own_hid = pltpu.make_async_copy(hidden_ref, raw, l_sem.at[1])
    own_hid.start()

    def weight_copy(c):
        return pltpu.make_async_copy(weight_ref.at[c], weff.at[c], w_sem.at[c])

    def start_weights(i):
        loop(p, lambda xx: weight_copy(order(i, high) * p + xx).start())

    loop(q, start_weights)

    barrier = pltpu.get_barrier_semaphore()

    def greet(device):
        pl.semaphore_signal(barrier, inc=1, device_id=device, device_id_type=MESH)

    for k in range(1, q):
        greet((wi, twin(k)))
    loop(p - 1, lambda r: greet(at_zx(z, (x + 1 + r) % p)))

    @pl.when(z > 0)
    def _():
        greet(at_zx(z - 1, x))

    @pl.when(z < q - 1)
    def _():
        greet(at_zx(z + 1, x))

    ends = (z == 0) | (z == q - 1)

    @pl.when(ends)
    def _():
        pl.semaphore_wait(barrier, q + p - 1)

    @pl.when(jnp.logical_not(ends))
    def _():
        pl.semaphore_wait(barrier, q + p)

    def ag_copy(k):
        return remote(grads.at[0], grads.at[k], ag_s.at[k], ag_r.at[k], (wi, twin(k)))

    def hid_copy(k):
        return remote(hid, hall_ref.at[k], hd_s.at[k], hd_r.at[k], (wi, twin(k)))

    def hid_here():
        return pltpu.make_async_copy(hid, hall_ref.at[0], l_sem.at[1])

    def share_hidden():
        own_hid.wait()
        groups, width = raw.shape[1:]

        def step(i):
            at = pl.ds(pl.multiple_of(i * 16, 16), 16)
            for g in range(groups):
                hid[at, g * width:(g + 1) * width] = raw[at, g, :]

        loop(raw.shape[0] // 16, step)
        for k in range(1, q):
            hid_copy(k).start()
        hid_here().start()

    own_grad.wait()
    for k in range(1, q):
        ag_copy(k).start()

    features = weff.shape[2]
    blocks = features // BLOCK
    row = lax.broadcasted_iota(jnp.int32, (blocks, features), 0)
    col = lax.broadcasted_iota(jnp.int32, (blocks, features), 1)
    low = row * BLOCK
    spread = jnp.where((col >= low) & (col < low + BLOCK), 1.0, 0.0).astype(BF16)
    s32[...] = lax.dot_general(
        scale_ref[...], spread, (((0,), (0,)), ((), ())), preferred_element_type=F32)

    units = weff.shape[1]
    per_chunk = units // BLOCK

    def scale_chunk(c):
        weight_copy(c).wait()

        def step(i):
            at = pl.ds(pl.multiple_of(i * BLOCK, BLOCK), BLOCK)
            factor = s32[pl.ds(c * per_chunk + i, 1), :]
            weff[c, at, :] = (weff[c, at, :].astype(F32) * factor).astype(BF16)

        loop(per_chunk, step, 4)

    def xa_copy(b, zt, r):
        xx = (x + 1 + r) % p
        return remote(pa.at[b, zt, xx], xr.at[b, zt, r], xa_s.at[b, zt, r], xa_r.at[b, zt, r], at_zx(z, xx))

    def ud_copy(d, b, zt):
        return remote(ud.at[d, b, zt], ud.at[d, b, zt], ud_s.at[d, b, zt], ud_r.at[d, b, zt],
                      at_zx(z + 1 - 2 * d, x))

    def ub_copy(d, b, zt, src):
        return remote(src, udb.at[d, b, zt], ub_s.at[d, b, zt], ub_r.at[d, b, zt],
                      at_zx(z + 1 - 2 * d, x))

    def send_row(b, zt):
        loop(p - 1, lambda r: xa_copy(b, zt, r).start())
        for d in range(2):
            @pl.when((z == d * (q - 1)) & (zt != z))
            def _():
                ub_copy(d, b, zt, pb.at[b, zt]).start()

    def keep(b, zt, xx, part):
        pa[b, zt, xx] = part[:ra]
        pb[b, zt, xx] = part[ra:]

    def first_rows(i):
        zt = order(i, high)

        def per_col(xx):
            c = zt * p + xx
            scale_chunk(c)
            keep(0, zt, xx, lax.dot_general(
                grads[0], weff[c], (((1,), (1,)), ((), ())), preferred_element_type=F32
            ).astype(BF16))

        loop(p, per_col)
        send_row(0, zt)

    def other_rows(i):
        zt = order(i, high)

        def per_col(xx):
            part = lax.dot_general(
                grads[1:].reshape((q - 1) * tokens, features), weff[zt * p + xx],
                (((1,), (1,)), ((), ())), preferred_element_type=F32).astype(BF16)
            for b in range(1, q):
                keep(b, zt, xx, part[(b - 1) * tokens:b * tokens])

        loop(p, per_col)
        send_row(1, zt)

    def wait_x(b, zt):
        loop(p - 1, lambda r: xa_copy(b, zt, r).wait_recv())

    def x_sources(b, zt):
        return [pa.at[b, zt, x]] + [xr.at[b, zt, r] for r in range(p - 1)]

    def stage_zb(b):
        for ph in range(2):
            d = (ph + high) % 2

            def step_b(i):
                zt = order(i, d)

                @pl.when(((zt - z) * (1 - 2 * d) > 0) & (z != d * (q - 1)))
                def _():
                    copy = ub_copy(d, b, zt, udb.at[d, b, zt])
                    copy.wait_recv()
                    loop(p, lambda xx: add_into(
                        udb.at[d, b, zt, xx], [udb.at[d, b, zt, xx], pb.at[b, zt, xx]], rb))
                    copy.start()

            loop(q, step_b)

    def stage_za(b):
        for ph in range(2):
            d = (ph + high) % 2
            edge = d * (q - 1)

            def step_a(i):
                zt = order(i, d)

                @pl.when((zt - z) * (1 - 2 * d) > 0)
                def _():
                    wait_x(b, zt)
                    copy = ud_copy(d, b, zt)

                    @pl.when(z != edge)
                    def _():
                        copy.wait_recv()
                        add_into(ud.at[d, b, zt], [ud.at[d, b, zt]] + x_sources(b, zt), ra)

                    @pl.when(z == edge)
                    def _():
                        add_into(ud.at[d, b, zt], x_sources(b, zt), ra)

                    copy.start()

            loop(q, step_a)

    def xb_copy(b, r):
        xx = (x + 1 + r) % p
        return remote(pb.at[b, z, xx], xrb.at[b, r], xb_s.at[b, r], xb_r.at[b, r], at_zx(z, xx))

    def stage_f1(b):
        for d in range(2):
            @pl.when(z != d * (q - 1))
            def _():
                ub_copy(d, b, z, udb.at[d, b, z]).wait_recv()
                loop(p, lambda xx: add_into(
                    pb.at[b, z, xx], [pb.at[b, z, xx], udb.at[d, b, z, xx]], rb))
        loop(p - 1, lambda r: xb_copy(b, r).start())

        wait_x(b, z)
        for d in range(2):
            @pl.when(z != d * (q - 1))
            def _():
                ud_copy(d, b, z).wait_recv()
        out = fin.at[b, pl.ds(0, ra)]

        @pl.when(z == 0)
        def _():
            add_into(out, x_sources(b, z) + [ud.at[1, b, z]], ra)

        @pl.when(z == q - 1)
        def _():
            add_into(out, x_sources(b, z) + [ud.at[0, b, z]], ra)

        @pl.when((z > 0) & (z < q - 1))
        def _():
            add_into(out, x_sources(b, z) + [ud.at[0, b, z], ud.at[1, b, z]], ra)

        share_out(b, 0)

    def fin_part(b, half):
        return fin.at[b, pl.ds(half * ra, rb if half else ra)]

    def gh_part(half):
        return gh_ref.at[n, pl.ds(half * ra, rb if half else ra)]

    def gh_copy(b, half):
        return remote(fin_part(b, half), gh_part(half), gh_s.at[half, b], gh_r.at[half, b], (wi, twin(b)))

    def gh_here(half):
        return pltpu.make_async_copy(fin_part(0, half), gh_part(half), gh_s.at[half, 0])

    def share_out(b, half):
        @pl.when(b == 0)
        def _():
            gh_here(half).start()

        @pl.when(b != 0)
        def _():
            gh_copy(b, half).start()

    def stage_f2(b):
        loop(p - 1, lambda r: xb_copy(b, r).wait_recv())
        add_into(fin_part(b, 1), [pb.at[b, z, x]] + [xrb.at[b, r] for r in range(p - 1)], rb)
        share_out(b, 1)

    def mz_copy(k, d, src):
        return remote(src, cols_ref.at[x, k], mz_s.at[d, k], mz_r.at[k], at_zx(z + 1 - 2 * d, x))

    def mx_copy(k, r, src):
        return remote(src, cols_ref.at[x, k], mx_s.at[k, r], mx_r.at[k, r], at_zx(z, (x + 1 + r) % p))

    def cols_here(k):
        return pltpu.make_async_copy(grads.at[k], cols_ref.at[x, k], own_sem.at[k])

    def multicast_source(k):
        @pl.when(z == n)
        def _():
            cols_here(k).start()
            for d in range(2):
                @pl.when(z != (1 - d) * (q - 1))
                def _():
                    mz_copy(k, d, grads.at[k]).start()

    def multicast_relay(k):
        @pl.when(z == n)
        def _():
            loop(p - 1, lambda r: mx_copy(k, r, grads.at[k]).start())

        for d in range(2):
            @pl.when((z - n) * (1 - 2 * d) > 0)
            def _():
                mz_copy(k, d, cols_ref.at[x, k]).wait_recv()

                @pl.when(z != (1 - d) * (q - 1))
                def _():
                    mz_copy(k, d, cols_ref.at[x, k]).start()

                loop(p - 1, lambda r: mx_copy(k, r, cols_ref.at[x, k]).start())

    multicast_source(0)
    ag_copy(q - 1).wait_recv()
    multicast_source(q - 1)
    loop(q, first_rows)
    for k in range(1, q - 1):
        ag_copy(k).wait_recv()
        multicast_source(k)
    loop(q, other_rows)
    loop(q - 2, lambda b: loop(q, lambda i: send_row(b + 2, order(i, high))))
    share_hidden()
    away = (z - n) * (z - n)
    inner = jnp.logical_not(ends)
    near = (away == 0) | (inner & (away == 1))

    def relay_early(condition):
        @pl.when(condition)
        def _():
            loop(2, lambda i: multicast_relay(i * (q - 1)))

    def relay_late(condition):
        @pl.when(condition)
        def _():
            loop(q - 2, lambda i: multicast_relay(i + 1))

    relay_early(near)
    loop(q, stage_zb)
    relay_late(near)
    relay_early(inner & (away > 1))

    def stage(s):
        stage_za(s)
        relay_late((s == 1) & inner & (away > 1))

        @pl.when(inner & (s >= 1))
        def _():
            stage_f1(s - 1)

    loop(q, stage)
    relay_early(ends & (away > 0))

    @pl.when(ends)
    def _():
        loop(q - 2, stage_f1)

    relay_late(ends & (away > 0))

    @pl.when(ends)
    def _():
        stage_f1(q - 2)

    loop(q - 1, stage_f2)
    stage_f1(q - 1)
    stage_f2(q - 1)

    for k in range(1, q):
        ag_copy(k).wait_send()
        hid_copy(k).wait()
        for half in range(2):
            gh_copy(k, half).wait()
    hid_here().wait()
    for half in range(2):
        gh_here(half).wait()

    def drain_b(b):
        loop(p - 1, lambda r: xb_copy(b, r).wait_send())

        def per_row(zt):
            loop(p - 1, lambda r: xa_copy(b, zt, r).wait_send())
            for d in range(2):
                @pl.when((zt - z) * (1 - 2 * d) > 0)
                def _():
                    ud_copy(d, b, zt).wait_send()
                    ub_copy(d, b, zt, udb.at[d, b, zt]).wait_send()

        loop(q, per_row)

        @pl.when(z == n)
        def _():
            cols_here(b).wait()

        for d in range(2):
            @pl.when(((z - n) * (1 - 2 * d) >= 0) & (z != (1 - d) * (q - 1)))
            def _():
                mz_copy(b, d, cols_ref.at[x, b]).wait_send()
        loop(p - 1, lambda r: mx_copy(b, r, cols_ref.at[x, b]).wait())

    loop(q, drain_b)


def exchange(wide, narrow, hidden, grad_out, weight, scale_t):
    q = narrow
    p = wide // narrow
    tokens, features = grad_out.shape
    units = weight.shape[1]
    ra = tokens * 3 // 4 // 16 * 16
    rb = tokens - ra
    flat = (tokens, hidden.shape[1] * hidden.shape[2])
    dma = pltpu.SemaphoreType.DMA
    any_space = pl.BlockSpec(memory_space=pl.ANY)
    vm = pl.BlockSpec(memory_space=pltpu.VMEM)
    return pl.pallas_call(
        functools.partial(exchange_kernel, q, p, ra),
        out_shape=(
            jax.ShapeDtypeStruct((narrow, tokens, units), BF16),
            jax.ShapeDtypeStruct((p, q, tokens, features), BF16),
            jax.ShapeDtypeStruct((q,) + flat, BF16),
        ),
        in_specs=[vm, any_space, any_space, any_space],
        out_specs=(any_space, any_space, any_space),
        scratch_shapes=[
            pltpu.VMEM((wide, units, features), BF16),
            pltpu.VMEM((scale_t.shape[1], features), F32),
            pltpu.VMEM((q, tokens, features), BF16),
            pltpu.VMEM(hidden.shape, BF16),
            pltpu.VMEM(flat, BF16),
            pltpu.VMEM((q, q, p, ra, units), BF16),
            pltpu.VMEM((q, q, p, rb, units), BF16),
            pltpu.VMEM((q, q, p - 1, ra, units), BF16),
            pltpu.VMEM((2, q, q, ra, units), BF16),
            pltpu.VMEM((2, q, q, p, rb, units), BF16),
            pltpu.VMEM((q, p - 1, rb, units), BF16),
            pltpu.VMEM((q, tokens, units), BF16),
            dma((wide,)), dma((2,)), dma((q,)), dma((q,)), dma((q,)), dma((q,)),
            dma((q, q, p - 1)), dma((q, q, p - 1)),
            dma((2, q, q)), dma((2, q, q)), dma((2, q, q)), dma((2, q, q)),
            dma((q, p - 1)), dma((q, p - 1)), dma((2, q)), dma((2, q)),
            dma((2, q)), dma((q,)), dma((q, p - 1)), dma((q, p - 1)), dma((q,)),
        ],
        compiler_params=pltpu.CompilerParams(
            collective_id=0, has_side_effects=True, vmem_limit_bytes=62 * 1024 * 1024),
        name="exchange",
    )(scale_t, weight, grad_out, hidden)


def outer_kernel(groups, units, cols_ref, hidden_ref, gh_ref, out_ref, grad_hidden_ref, rows_ref):
    rows = cols_ref.shape[2]
    for g in range(groups):
        part = lax.dot_general(
            cols_ref[0], hidden_ref[:, g * units:(g + 1) * units],
            (((0,), (0,)), ((), ())), preferred_element_type=F32)
        for j in range(units // 128):
            rows_ref[j, pl.ds(g, rows, stride=groups), :] = part[:, j * 128:(j + 1) * 128]
    for j in range(units // 128):
        out_ref[:, :, j * 128:(j + 1) * 128] = rows_ref[j].astype(BF16).reshape(rows, groups, 128)
    for g in range(groups):
        grad_hidden_ref[:, g, :] = gh_ref[g]


def outer_product(cols, hidden, gh):
    p, tokens, features = cols.shape
    groups, own, units = gh.shape
    rows = min(256, features)
    steps = features // rows
    share = own // (p * steps)
    return pl.pallas_call(
        functools.partial(outer_kernel, groups, units),
        grid=(p, steps),
        out_shape=(
            jax.ShapeDtypeStruct((p * features, groups, units), BF16),
            jax.ShapeDtypeStruct((own, groups, units), BF16),
        ),
        in_specs=[
            pl.BlockSpec((1, tokens, rows), lambda i, j: (i, 0, j)),
            pl.BlockSpec(hidden.shape, lambda i, j: (0, 0), pipeline_mode=pl.Buffered(1)),
            pl.BlockSpec((groups, share, units), lambda i, j: (0, i * steps + j, 0)),
        ],
        out_specs=(
            pl.BlockSpec((rows, groups, units), lambda i, j: (i * steps + j, 0, 0)),
            pl.BlockSpec((share, groups, units), lambda i, j: (i * steps + j, 0, 0)),
        ),
        scratch_shapes=[pltpu.VMEM((units // 128, rows * groups, 128), F32)],
        compiler_params=pltpu.CompilerParams(vmem_limit_bytes=60 * 1024 * 1024),
        name="outer_product",
    )(cols, hidden, gh)


def per_device(wide, narrow, hidden, grad_out, weight_base, block_scale):
    tokens, groups, units = hidden.shape
    features = grad_out.shape[1]
    weight = weight_base.reshape(wide, weight_base.shape[0] // wide, features)
    gh, cols, hall = exchange(wide, narrow, hidden, grad_out, weight, block_scale.T)
    p = cols.shape[0]
    every = narrow * tokens
    grad_weight, grad_hidden = outer_product(
        cols.reshape(p, every, features), hall.reshape(every, groups * units), gh)
    return grad_hidden, grad_weight


def solution(mesh):
    wide, narrow = mesh.shape["wide"], mesh.shape["narrow"]
    return jax.shard_map(
        functools.partial(per_device, wide, narrow),
        mesh=mesh,
        in_specs=(P("narrow", None, "wide"), P("narrow", "wide"), P("narrow", "wide"), P("narrow", "wide")),
        out_specs=(P("narrow", None, "wide"), P("narrow", None, "wide")),
        check_vma=False,
    )
```

```python
import functools

import jax
import jax.numpy as jnp
from jax import lax
from jax.experimental import pallas as pl
from jax.experimental.pallas import tpu as pltpu
from jax.sharding import PartitionSpec as P

MESH = pl.DeviceIdType.MESH
BLOCK = 16
F32 = jnp.float32
BF16 = jnp.bfloat16


def loop(count, body, unroll=1):
    def step(i, carry):
        body(i)
        return carry

    lax.fori_loop(0, count, step, 0, unroll=unroll)


def add_into(dst, sources, rows):
    def step(i):
        at = pl.ds(pl.multiple_of(i * 16, 16), 16)
        total = sources[0][at, :].astype(F32)
        for source in sources[1:]:
            total = total + source[at, :].astype(F32)
        dst[at, :] = total.astype(BF16)

    loop(rows // 16, step)


def exchange_kernel(
    q, p, ra, scale_ref, weight_ref, grad_ref, hidden_ref,
    gh_ref, cols_ref, hall_ref,
    weff, s32, grads, raw, hid, pa, pb, xr, ud, udb, xrb, fin,
    w_sem, l_sem, ag_s, ag_r, hd_s, hd_r, xa_s, xa_r, ud_s, ud_r, ub_s, ub_r,
    xb_s, xb_r, gh_s, gh_r, mz_s, mz_r, mx_s, mx_r, own_sem,
):
    wide = q * p
    wi = lax.axis_index("wide")
    n = lax.axis_index("narrow")
    z = wi // p
    x = wi % p
    tokens = grads.shape[1]
    rb = tokens - ra
    high = (2 * z) // q

    def twin(k):
        a, b = k // 2, (k % 2 + k // 2) % 2
        return ((n % 2 + a) % 2) + 2 * ((n // 2 + b) % 2)

    def remote(src, dst, send, recv, to):
        return pltpu.make_async_remote_copy(
            src_ref=src, dst_ref=dst, send_sem=send, recv_sem=recv,
            device_id=to, device_id_type=MESH)

    def at_zx(zz, xx):
        return (zz * p + xx, n)

    def order(i, d):
        return i + (1 - d) * (q - 1 - 2 * i)

    own_grad = pltpu.make_async_copy(grad_ref, grads.at[0], l_sem.at[0])
    own_grad.start()
    own_hid = pltpu.make_async_copy(hidden_ref, raw, l_sem.at[1])
    own_hid.start()

    def weight_copy(c):
        return pltpu.make_async_copy(weight_ref.at[c], weff.at[c], w_sem.at[c])

    def start_weights(i):
        loop(p, lambda xx: weight_copy(order(i, high) * p + xx).start())

    loop(q, start_weights)

    barrier = pltpu.get_barrier_semaphore()

    def greet(device):
        pl.semaphore_signal(barrier, inc=1, device_id=device, device_id_type=MESH)

    for k in range(1, q):
        greet((wi, twin(k)))
    loop(p - 1, lambda r: greet(at_zx(z, (x + 1 + r) % p)))

    @pl.when(z > 0)
    def _():
        greet(at_zx(z - 1, x))

    @pl.when(z < q - 1)
    def _():
        greet(at_zx(z + 1, x))

    ends = (z == 0) | (z == q - 1)

    @pl.when(ends)
    def _():
        pl.semaphore_wait(barrier, q + p - 1)

    @pl.when(jnp.logical_not(ends))
    def _():
        pl.semaphore_wait(barrier, q + p)

    def ag_copy(k):
        return remote(grads.at[0], grads.at[k], ag_s.at[k], ag_r.at[k], (wi, twin(k)))

    def hid_copy(k):
        return remote(hid, hall_ref.at[k], hd_s.at[k], hd_r.at[k], (wi, twin(k)))

    def hid_here():
        return pltpu.make_async_copy(hid, hall_ref.at[0], l_sem.at[1])

    def share_hidden():
        own_hid.wait()
        groups, width = raw.shape[1:]

        def step(i):
            at = pl.ds(pl.multiple_of(i * 16, 16), 16)
            for g in range(groups):
                hid[at, g * width:(g + 1) * width] = raw[at, g, :]

        loop(raw.shape[0] // 16, step)
        for k in range(1, q):
            hid_copy(k).start()
        hid_here().start()

    own_grad.wait()
    for k in range(1, q):
        ag_copy(k).start()

    features = weff.shape[2]
    blocks = features // BLOCK
    row = lax.broadcasted_iota(jnp.int32, (blocks, features), 0)
    col = lax.broadcasted_iota(jnp.int32, (blocks, features), 1)
    low = row * BLOCK
    spread = jnp.where((col >= low) & (col < low + BLOCK), 1.0, 0.0).astype(BF16)
    s32[...] = lax.dot_general(
        scale_ref[...], spread, (((0,), (0,)), ((), ())), preferred_element_type=F32)

    units = weff.shape[1]
    per_chunk = units // BLOCK

    def scale_chunk(c):
        weight_copy(c).wait()

        def step(i):
            at = pl.ds(pl.multiple_of(i * BLOCK, BLOCK), BLOCK)
            factor = s32[pl.ds(c * per_chunk + i, 1), :]
            weff[c, at, :] = (weff[c, at, :].astype(F32) * factor).astype(BF16)

        loop(per_chunk, step, 4)

    def xa_copy(b, zt, r):
        xx = (x + 1 + r) % p
        return remote(pa.at[b, zt, xx], xr.at[b, zt, r], xa_s.at[b, zt, r], xa_r.at[b, zt, r], at_zx(z, xx))

    def ud_copy(d, b, zt):
        return remote(ud.at[d, b, zt], ud.at[d, b, zt], ud_s.at[d, b, zt], ud_r.at[d, b, zt],
                      at_zx(z + 1 - 2 * d, x))

    def ub_copy(d, b, zt, src):
        return remote(src, udb.at[d, b, zt], ub_s.at[d, b, zt], ub_r.at[d, b, zt],
                      at_zx(z + 1 - 2 * d, x))

    def send_ends(b, zt):
        for d in range(2):
            @pl.when((z == d * (q - 1)) & (zt != z))
            def _():
                ub_copy(d, b, zt, pb.at[b, zt]).start()

    def send_row(b, zt):
        loop(p - 1, lambda r: xa_copy(b, zt, r).start())
        send_ends(b, zt)

    def keep(b, zt, xx, part):
        pa[b, zt, xx] = part[:ra]
        pb[b, zt, xx] = part[ra:]

    def first_rows(i):
        zt = order(i, high)

        def per_col(r):
            xx = (x + 1 + r) % p
            c = zt * p + xx
            scale_chunk(c)
            keep(0, zt, xx, lax.dot_general(
                grads[0], weff[c], (((1,), (1,)), ((), ())), preferred_element_type=F32
            ).astype(BF16))

            @pl.when(r < p - 1)
            def _():
                xa_copy(0, zt, r).start()

        loop(p, per_col)
        send_ends(0, zt)

    def other_rows(i):
        zt = order(i, high)

        def per_col(xx):
            part = lax.dot_general(
                grads[1:].reshape((q - 1) * tokens, features), weff[zt * p + xx],
                (((1,), (1,)), ((), ())), preferred_element_type=F32).astype(BF16)
            for b in range(1, q):
                keep(b, zt, xx, part[(b - 1) * tokens:b * tokens])

        loop(p, per_col)
        send_row(1, zt)

    def wait_x(b, zt):
        loop(p - 1, lambda r: xa_copy(b, zt, r).wait_recv())

    def x_sources(b, zt):
        return [pa.at[b, zt, x]] + [xr.at[b, zt, r] for r in range(p - 1)]

    def stage_zb(b):
        for ph in range(2):
            d = (ph + high) % 2

            def step_b(i):
                zt = order(i, d)

                @pl.when(((zt - z) * (1 - 2 * d) > 0) & (z != d * (q - 1)))
                def _():
                    copy = ub_copy(d, b, zt, udb.at[d, b, zt])
                    copy.wait_recv()
                    loop(p, lambda xx: add_into(
                        udb.at[d, b, zt, xx], [udb.at[d, b, zt, xx], pb.at[b, zt, xx]], rb))
                    copy.start()

            loop(q, step_b)

    def stage_za(b):
        for ph in range(2):
            d = (ph + high) % 2
            edge = d * (q - 1)

            def step_a(i):
                zt = order(i, d)

                @pl.when((zt - z) * (1 - 2 * d) > 0)
                def _():
                    wait_x(b, zt)
                    copy = ud_copy(d, b, zt)

                    @pl.when(z != edge)
                    def _():
                        copy.wait_recv()
                        add_into(ud.at[d, b, zt], [ud.at[d, b, zt]] + x_sources(b, zt), ra)

                    @pl.when(z == edge)
                    def _():
                        add_into(ud.at[d, b, zt], x_sources(b, zt), ra)

                    copy.start()

            loop(q, step_a)

    def xb_copy(b, r):
        xx = (x + 1 + r) % p
        return remote(pb.at[b, z, xx], xrb.at[b, r], xb_s.at[b, r], xb_r.at[b, r], at_zx(z, xx))

    def stage_f1(b):
        for d in range(2):
            @pl.when(z != d * (q - 1))
            def _():
                ub_copy(d, b, z, udb.at[d, b, z]).wait_recv()
                loop(p, lambda xx: add_into(
                    pb.at[b, z, xx], [pb.at[b, z, xx], udb.at[d, b, z, xx]], rb))
        loop(p - 1, lambda r: xb_copy(b, r).start())

        wait_x(b, z)
        for d in range(2):
            @pl.when(z != d * (q - 1))
            def _():
                ud_copy(d, b, z).wait_recv()
        out = fin.at[b, pl.ds(0, ra)]

        @pl.when(z == 0)
        def _():
            add_into(out, x_sources(b, z) + [ud.at[1, b, z]], ra)

        @pl.when(z == q - 1)
        def _():
            add_into(out, x_sources(b, z) + [ud.at[0, b, z]], ra)

        @pl.when((z > 0) & (z < q - 1))
        def _():
            add_into(out, x_sources(b, z) + [ud.at[0, b, z], ud.at[1, b, z]], ra)

        share_out(b, 0)

    def fin_part(b, half):
        return fin.at[b, pl.ds(half * ra, rb if half else ra)]

    def gh_part(half):
        return gh_ref.at[n, pl.ds(half * ra, rb if half else ra)]

    def gh_copy(b, half):
        return remote(fin_part(b, half), gh_part(half), gh_s.at[half, b], gh_r.at[half, b], (wi, twin(b)))

    def gh_here(half):
        return pltpu.make_async_copy(fin_part(0, half), gh_part(half), gh_s.at[half, 0])

    def share_out(b, half):
        @pl.when(b == 0)
        def _():
            gh_here(half).start()

        @pl.when(b != 0)
        def _():
            gh_copy(b, half).start()

    def stage_f2(b):
        loop(p - 1, lambda r: xb_copy(b, r).wait_recv())
        add_into(fin_part(b, 1), [pb.at[b, z, x]] + [xrb.at[b, r] for r in range(p - 1)], rb)
        share_out(b, 1)

    def mz_copy(k, d, src):
        return remote(src, cols_ref.at[x, k], mz_s.at[d, k], mz_r.at[k], at_zx(z + 1 - 2 * d, x))

    def mx_copy(k, r, src):
        return remote(src, cols_ref.at[x, k], mx_s.at[k, r], mx_r.at[k, r], at_zx(z, (x + 1 + r) % p))

    def cols_here(k):
        return pltpu.make_async_copy(grads.at[k], cols_ref.at[x, k], own_sem.at[k])

    def multicast_source(k):
        @pl.when(z == n)
        def _():
            cols_here(k).start()
            for d in range(2):
                @pl.when(z != (1 - d) * (q - 1))
                def _():
                    mz_copy(k, d, grads.at[k]).start()

    def multicast_relay(k):
        @pl.when(z == n)
        def _():
            loop(p - 1, lambda r: mx_copy(k, r, grads.at[k]).start())

        for d in range(2):
            @pl.when((z - n) * (1 - 2 * d) > 0)
            def _():
                mz_copy(k, d, cols_ref.at[x, k]).wait_recv()

                @pl.when(z != (1 - d) * (q - 1))
                def _():
                    mz_copy(k, d, cols_ref.at[x, k]).start()

                loop(p - 1, lambda r: mx_copy(k, r, cols_ref.at[x, k]).start())

    multicast_source(0)
    ag_copy(q - 1).wait_recv()
    multicast_source(q - 1)
    loop(q, first_rows)
    for k in range(1, q - 1):
        ag_copy(k).wait_recv()
        multicast_source(k)
    loop(q, other_rows)
    loop(q - 2, lambda b: loop(q, lambda i: send_row(b + 2, order(i, high))))
    share_hidden()
    away = (z - n) * (z - n)
    inner = jnp.logical_not(ends)
    near = (away == 0) | (inner & (away == 1))

    def relay_early(condition):
        @pl.when(condition)
        def _():
            loop(2, lambda i: multicast_relay(i * (q - 1)))

    def relay_late(condition):
        @pl.when(condition)
        def _():
            loop(q - 2, lambda i: multicast_relay(i + 1))

    relay_early(near)
    loop(q, stage_zb)
    relay_late(near)
    relay_early(inner & (away > 1))

    def stage(s):
        stage_za(s)
        relay_late((s == 1) & inner & (away > 1))

        @pl.when(inner & (s >= 1))
        def _():
            stage_f1(s - 1)

    loop(q, stage)
    relay_early(ends & (away > 0))

    @pl.when(ends)
    def _():
        loop(q - 2, stage_f1)

    relay_late(ends & (away > 0))

    @pl.when(ends)
    def _():
        stage_f1(q - 2)

    loop(q - 1, stage_f2)
    stage_f1(q - 1)
    stage_f2(q - 1)

    for k in range(1, q):
        ag_copy(k).wait_send()
        hid_copy(k).wait()
        for half in range(2):
            gh_copy(k, half).wait()
    hid_here().wait()
    for half in range(2):
        gh_here(half).wait()

    def drain_b(b):
        loop(p - 1, lambda r: xb_copy(b, r).wait_send())

        def per_row(zt):
            loop(p - 1, lambda r: xa_copy(b, zt, r).wait_send())
            for d in range(2):
                @pl.when((zt - z) * (1 - 2 * d) > 0)
                def _():
                    ud_copy(d, b, zt).wait_send()
                    ub_copy(d, b, zt, udb.at[d, b, zt]).wait_send()

        loop(q, per_row)

        @pl.when(z == n)
        def _():
            cols_here(b).wait()

        for d in range(2):
            @pl.when(((z - n) * (1 - 2 * d) >= 0) & (z != (1 - d) * (q - 1)))
            def _():
                mz_copy(b, d, cols_ref.at[x, b]).wait_send()
        loop(p - 1, lambda r: mx_copy(b, r, cols_ref.at[x, b]).wait())

    loop(q, drain_b)


def exchange(wide, narrow, hidden, grad_out, weight, scale_t):
    q = narrow
    p = wide // narrow
    tokens, features = grad_out.shape
    units = weight.shape[1]
    ra = tokens * 3 // 4 // 16 * 16
    rb = tokens - ra
    flat = (tokens, hidden.shape[1] * hidden.shape[2])
    dma = pltpu.SemaphoreType.DMA
    any_space = pl.BlockSpec(memory_space=pl.ANY)
    vm = pl.BlockSpec(memory_space=pltpu.VMEM)
    return pl.pallas_call(
        functools.partial(exchange_kernel, q, p, ra),
        out_shape=(
            jax.ShapeDtypeStruct((narrow, tokens, units), BF16),
            jax.ShapeDtypeStruct((p, q, tokens, features), BF16),
            jax.ShapeDtypeStruct((q,) + flat, BF16),
        ),
        in_specs=[vm, any_space, any_space, any_space],
        out_specs=(any_space, any_space, any_space),
        scratch_shapes=[
            pltpu.VMEM((wide, units, features), BF16),
            pltpu.VMEM((scale_t.shape[1], features), F32),
            pltpu.VMEM((q, tokens, features), BF16),
            pltpu.VMEM(hidden.shape, BF16),
            pltpu.VMEM(flat, BF16),
            pltpu.VMEM((q, q, p, ra, units), BF16),
            pltpu.VMEM((q, q, p, rb, units), BF16),
            pltpu.VMEM((q, q, p - 1, ra, units), BF16),
            pltpu.VMEM((2, q, q, ra, units), BF16),
            pltpu.VMEM((2, q, q, p, rb, units), BF16),
            pltpu.VMEM((q, p - 1, rb, units), BF16),
            pltpu.VMEM((q, tokens, units), BF16),
            dma((wide,)), dma((2,)), dma((q,)), dma((q,)), dma((q,)), dma((q,)),
            dma((q, q, p - 1)), dma((q, q, p - 1)),
            dma((2, q, q)), dma((2, q, q)), dma((2, q, q)), dma((2, q, q)),
            dma((q, p - 1)), dma((q, p - 1)), dma((2, q)), dma((2, q)),
            dma((2, q)), dma((q,)), dma((q, p - 1)), dma((q, p - 1)), dma((q,)),
        ],
        compiler_params=pltpu.CompilerParams(
            collective_id=0, has_side_effects=True, vmem_limit_bytes=62 * 1024 * 1024),
        name="exchange",
    )(scale_t, weight, grad_out, hidden)


def outer_kernel(groups, units, cols_ref, hidden_ref, gh_ref, out_ref, grad_hidden_ref, rows_ref):
    rows = cols_ref.shape[2]
    for g in range(groups):
        part = lax.dot_general(
            cols_ref[0], hidden_ref[:, g * units:(g + 1) * units],
            (((0,), (0,)), ((), ())), preferred_element_type=F32)
        for j in range(units // 128):
            rows_ref[j, pl.ds(g, rows, stride=groups), :] = part[:, j * 128:(j + 1) * 128]
    for j in range(units // 128):
        out_ref[:, :, j * 128:(j + 1) * 128] = rows_ref[j].astype(BF16).reshape(rows, groups, 128)
    for g in range(groups):
        grad_hidden_ref[:, g, :] = gh_ref[g]


def outer_product(cols, hidden, gh):
    p, tokens, features = cols.shape
    groups, own, units = gh.shape
    rows = min(256, features)
    steps = features // rows
    share = own // (p * steps)
    return pl.pallas_call(
        functools.partial(outer_kernel, groups, units),
        grid=(p, steps),
        out_shape=(
            jax.ShapeDtypeStruct((p * features, groups, units), BF16),
            jax.ShapeDtypeStruct((own, groups, units), BF16),
        ),
        in_specs=[
            pl.BlockSpec((1, tokens, rows), lambda i, j: (i, 0, j)),
            pl.BlockSpec(hidden.shape, lambda i, j: (0, 0), pipeline_mode=pl.Buffered(1)),
            pl.BlockSpec((groups, share, units), lambda i, j: (0, i * steps + j, 0)),
        ],
        out_specs=(
            pl.BlockSpec((rows, groups, units), lambda i, j: (i * steps + j, 0, 0)),
            pl.BlockSpec((share, groups, units), lambda i, j: (i * steps + j, 0, 0)),
        ),
        scratch_shapes=[pltpu.VMEM((units // 128, rows * groups, 128), F32)],
        compiler_params=pltpu.CompilerParams(vmem_limit_bytes=60 * 1024 * 1024),
        name="outer_product",
    )(cols, hidden, gh)


def per_device(wide, narrow, hidden, grad_out, weight_base, block_scale):
    tokens, groups, units = hidden.shape
    features = grad_out.shape[1]
    weight = weight_base.reshape(wide, weight_base.shape[0] // wide, features)
    gh, cols, hall = exchange(wide, narrow, hidden, grad_out, weight, block_scale.T)
    p = cols.shape[0]
    every = narrow * tokens
    grad_weight, grad_hidden = outer_product(
        cols.reshape(p, every, features), hall.reshape(every, groups * units), gh)
    return grad_hidden, grad_weight


def solution(mesh):
    wide, narrow = mesh.shape["wide"], mesh.shape["narrow"]
    return jax.shard_map(
        functools.partial(per_device, wide, narrow),
        mesh=mesh,
        in_specs=(P("narrow", None, "wide"), P("narrow", "wide"), P("narrow", "wide"), P("narrow", "wide")),
        out_specs=(P("narrow", None, "wide"), P("narrow", None, "wide")),
        check_vma=False,
    )
```
